32 devices in a mesh: dp: 8 (over y, x, core), seq: 4 (over z).
Axes of the slice: x: 2, y: 2, z: 4, core: 2. Of those that a mesh axis runs over, the one named last changes fastest.
Arguments:
- query_rows: bfloat16 [8, 512, 3072], P('dp', 'seq'), may hold values from -6 to 6
- key_rows: bfloat16 [8, 512, 3072], P('dp', 'seq'), may hold values from -6 to 6
- value_rows: bfloat16 [8, 512, 3072], P('dp', 'seq'), may hold values from -6 to 6
- out_grad: bfloat16 [8, 512, 6144], P('dp', 'seq'), may hold values from -54 to 54
- clip_lengths: int32 [8, 4], P('dp'), may hold values from 1 to 256, 512 in all within a row
- out_weight: bfloat16 [3072, 6144], P('seq'), may hold values from -0.109375 to 0.109375
- query_gain: float32 [128], replicated, may hold values from 0.1 to 1.9
- key_gain: float32 [128], replicated, may hold values from 0.1 to 1.9
Outputs:
- query_grad: bfloat16 [8, 512, 3072], P('dp', 'seq')
- key_grad: bfloat16 [8, 512, 3072], P('dp', 'seq')
- value_grad: bfloat16 [8, 512, 3072], P('dp', 'seq')
- weight_grad: float32 [3072, 6144], P('seq', 'dp')
- querygain_grad: float32 [128], replicated
- keygain_grad: float32 [128], replicated
- grad_norm: float32 [], replicated
The draws below stay inside these ranges and needn't reach their ends.
Inputs may be any that keep to these rules, and one draw needn't show every extreme that they name: `clip_lengths`: the token counts of each group's clips sum to 512.
All inputs are finite; a program needn't handle non-finite values.
Results may differ from the reference program's by a relative error of at most 0.015.
Values may be sent and summed in bfloat16 or wider, within the bound.
A program may use at most 128 MiB of HBM per device.

```python
import math
import jax
import jax.numpy as jnp
import numpy as np
from jax import lax

D = 6144
HEAD_DIM = 128
CLIPS = 4
GROUPS = 8
SEQ_LEN = 512
INNER = 3072
MAX_NORM = 768


def draw_out_grad(key, part):
    first = jax.random.fold_in(key, 0)
    second = jax.random.fold_in(key, 1)
    fifth = jax.random.fold_in(key, 4)
    row_scale = jnp.exp(jax.random.uniform(first, (GROUPS, SEQ_LEN, 1), jnp.float32, -1.2, 1.1))
    ramp = 0.5 + jnp.arange(D, dtype=jnp.float32) / (D - 1)
    column_scale = ramp * jnp.exp(jax.random.uniform(second, (D,), jnp.float32, -1.2, 1.1))
    base = jax.random.truncated_normal(fifth, -4.0, 4.0, (GROUPS, SEQ_LEN, D), jnp.float32)
    return (row_scale * column_scale * base).astype(jnp.bfloat16)


def block_scale(rng, dims, shards, smallest, top_value):
    loudness = 1.0
    for dim, blocks in shards:
        steps = jax.random.uniform(jax.random.fold_in(jax.random.fold_in(rng, 6), dim), (blocks,), jnp.float32, smallest / len(shards), top_value / len(shards))
        loudness = loudness * jnp.repeat(jnp.exp(steps), dims[dim] // blocks).reshape((-1,) + (1,) * (len(dims) - 1 - dim))
    return loudness


def length_profile(number_of, total, most, lean):
    loads = [(1 << 20) // math.isqrt(standing ** lean) + 1 for standing in range(2, number_of + 1)]
    rest, holding = total - most - (number_of - 1), [1] * (number_of - 1)
    while rest > 0:
        free = [i for i in range(number_of - 1) if holding[i] < most]
        pool, remaining = sum([loads[i] for i in free]), rest
        for i in free:
            addition = min(most - holding[i], max(1, remaining * loads[i] // pool), rest)
            holding[i] = holding[i] + addition
            rest = rest - addition
    return np.array([most] + holding)


def ragged_sizes(own_key, amount, total, bound, slope):
    if amount == 2:
        one = jax.random.randint(own_key, (), max(1, total - bound), min(bound, total - 1) + 1)
        return jnp.stack([one, total - one])
    sizes = jnp.asarray(length_profile(amount, total, bound, slope), jnp.int32)
    couples = (amount - 1) // 2
    giver, receiver = sizes[1:1 + 2 * couples:2], sizes[2:2 + 2 * couples:2]
    room = jnp.minimum(giver - 1, bound - receiver)
    passed = jax.random.randint(jax.random.fold_in(own_key, 1), (couples,), 0, 1 << 20) % (room + 1)
    sizes = sizes.at[1:1 + 2 * couples:2].set(giver - passed).at[2:2 + 2 * couples:2].set(receiver + passed)
    return sizes[jax.random.permutation(jax.random.fold_in(own_key, 2), amount)]


def bell_draw(own_key, shape, scale, limit, cuts=(), held_as=jnp.bfloat16):
    values = jax.random.normal(own_key, shape, jnp.float32) * scale
    if len(cuts) > 0:
        values = block_scale(own_key, shape, cuts, -0.22, 0.18) * values
    return jnp.clip(values, min=-limit, max=limit).astype(held_as)


def setup_inputs(seed: int = 0) -> dict:
    splits = jax.random.split(jax.random.key(seed), 9)
    return {
        "query_rows": bell_draw(splits[0], (GROUPS, SEQ_LEN, INNER), 1.0, 6.0, ((0, 8), (1, 4))),
        "key_rows": bell_draw(splits[1], (GROUPS, SEQ_LEN, INNER), 1.0, 6.0, ((0, 8), (1, 4))),
        "value_rows": bell_draw(splits[2], (GROUPS, SEQ_LEN, INNER), 1.0, 6.0, ((0, 8), (1, 4))),
        "out_grad": draw_out_grad(jax.random.fold_in(splits[8], 71), 0),
        "clip_lengths": jax.vmap(lambda own: ragged_sizes(own, CLIPS, SEQ_LEN, SEQ_LEN // 2, 2))(jax.random.split(splits[4], GROUPS)).reshape((GROUPS, CLIPS)).astype(jnp.int32),
        "out_weight": bell_draw(splits[5], (INNER, D), INNER ** -0.5, 0.109375, ((0, 4),)),
        "query_gain": jnp.clip(1.0 + 0.18 * jax.random.normal(splits[6], (HEAD_DIM,), jnp.float32), 0.1, 1.9),
        "key_gain": jnp.clip(1.0 + 0.18 * jax.random.normal(splits[7], (HEAD_DIM,), jnp.float32), 0.1, 1.9),
    }


EPS = 1e-06

def segment_ids(lengths, total):
    ends = jnp.cumsum(lengths.astype(jnp.int32))
    places = jnp.arange(total, dtype=jnp.int32)
    return lax.optimization_barrier(jnp.sum((places[:, None] >= ends[None, :]).astype(jnp.int32), axis=1)).astype(jnp.int32)

def norm_rows(rows, gain):
    wide = rows.astype(jnp.float32)
    inverse = lax.rsqrt(lax.optimization_barrier(jnp.mean(wide * wide, axis=-1, keepdims=True)) + EPS)
    unit = wide * inverse
    return (unit, inverse, (unit * gain).astype(jnp.bfloat16))

def norm_back(unit, inverse, gain, d_norm):
    gain_part = lax.optimization_barrier(jnp.sum(unit * d_norm, axis=(0, 1)))
    d_unit = d_norm * gain
    d_rows = inverse * (d_unit - unit * lax.optimization_barrier(jnp.mean(unit * d_unit, axis=-1, keepdims=True)))
    return (d_rows.astype(jnp.bfloat16), gain_part)

def one_group(query, keys, values, d_out, lengths, out_weight, query_gain, key_gain):
    total = query.shape[0]
    heads = query.shape[1] // HEAD_DIM
    scale = HEAD_DIM ** (-0.5)
    query3 = query.reshape(total, heads, HEAD_DIM)
    keys3 = keys.reshape(total, heads, HEAD_DIM)
    values3 = values.reshape(total, heads, HEAD_DIM).astype(jnp.float32)
    seg = segment_ids(lengths, total)
    same = seg[:, None] == seg[None, :]
    q_unit, q_inv, q_norm = norm_rows(query3, query_gain)
    k_unit, k_inv, k_norm = norm_rows(keys3, key_gain)
    scores = jnp.einsum('qhd,khd->hqk', q_norm.astype(jnp.float32), k_norm.astype(jnp.float32)) * scale
    expo = jnp.where(same[None], jnp.exp(scores), 0.0)
    probs = (expo / lax.optimization_barrier(jnp.sum(expo, axis=-1, keepdims=True))).astype(jnp.bfloat16)
    probs32 = probs.astype(jnp.float32)
    attn_out = jnp.einsum('hqk,khd->qhd', probs32, values3).astype(jnp.bfloat16)
    attn_flat = attn_out.reshape(total, heads * HEAD_DIM)
    weight_part = jnp.dot(attn_flat.T, d_out, preferred_element_type=jnp.float32)
    d_attn = jnp.dot(d_out, out_weight.T, preferred_element_type=jnp.float32).astype(jnp.bfloat16)
    d_attn32 = d_attn.reshape(total, heads, HEAD_DIM).astype(jnp.float32)
    d_probs = jnp.einsum('qhd,khd->hqk', d_attn32, values3)
    row_sum = lax.optimization_barrier(jnp.sum(probs32 * d_probs, axis=-1, keepdims=True))
    d_scores = (probs32 * (d_probs - row_sum) * scale).astype(jnp.bfloat16).astype(jnp.float32)
    value_grad = jnp.einsum('hqk,qhd->khd', probs32, d_attn32).astype(jnp.bfloat16)
    d_qnorm = jnp.einsum('hqk,khd->qhd', d_scores, k_norm.astype(jnp.float32))
    d_knorm = jnp.einsum('hqk,qhd->khd', d_scores, q_norm.astype(jnp.float32))
    query_grad, q_gain_part = norm_back(q_unit, q_inv, query_gain, d_qnorm)
    key_grad, k_gain_part = norm_back(k_unit, k_inv, key_gain, d_knorm)
    width = heads * HEAD_DIM
    return (query_grad.reshape(total, width), key_grad.reshape(total, width), value_grad.reshape(total, width), weight_part, q_gain_part, k_gain_part)

def reference(query_rows, key_rows, value_rows, out_grad, clip_lengths, out_weight, query_gain, key_gain):

    def step(carry, items):
        weight_sum, q_gain_sum, k_gain_sum = carry
        query, keys, values, d_out, lengths = items
        q_grad, k_grad, v_grad, weight_part, q_part, k_part = one_group(query, keys, values, d_out, lengths, out_weight, query_gain, key_gain)
        return ((weight_sum + weight_part, q_gain_sum + q_part, k_gain_sum + k_part), (q_grad, k_grad, v_grad))
    start = (jnp.zeros(out_weight.shape, jnp.float32), jnp.zeros((HEAD_DIM,), jnp.float32), jnp.zeros((HEAD_DIM,), jnp.float32))
    (weight_raw, qgain_raw, kgain_raw), (query_grad, key_grad, value_grad) = lax.scan(step, start, (query_rows, key_rows, value_rows, out_grad, clip_lengths))
    squares = jnp.sum(weight_raw * weight_raw) + jnp.sum(qgain_raw * qgain_raw) + jnp.sum(kgain_raw * kgain_raw)
    grad_norm = jnp.sqrt(squares)
    factor = jnp.minimum(jnp.float32(1.0), MAX_NORM / (grad_norm + EPS))
    return (query_grad, key_grad, value_grad, weight_raw * factor, qgain_raw * factor, kgain_raw * factor, grad_norm)
```

```python
import functools

import jax
import jax.numpy as jnp
from jax import lax
from jax.experimental import pallas as pl
from jax.experimental.pallas import tpu as pltpu
from jax.sharding import PartitionSpec as P

HEAD_DIM = 128
MAX_NORM = 768
EPS = 1e-06
CHUNKS = 4
SCALE = HEAD_DIM ** (-0.5)
NT = (((1,), (1,)), ((), ()))
TN = (((0,), (0,)), ((), ()))
NN = (((1,), (0,)), ((), ()))


def mm(a, b, dims):
    return lax.dot_general(a, b, dims, preferred_element_type=jnp.float32)


def segment_ids(lengths, total):
    ends = jnp.cumsum(lengths)
    places = jnp.arange(total, dtype=jnp.int32)
    return jnp.sum((places[:, None] >= ends[None, :]).astype(jnp.int32), axis=1)


def unit_rows(rows):
    wide = rows.astype(jnp.float32)
    inverse = lax.rsqrt(jnp.mean(wide * wide, axis=-1, keepdims=True) + EPS)
    return wide * inverse, inverse


def probs_of(qn, kn, same):
    scores = mm(qn, kn, NT) * SCALE
    expo = jnp.where(same, jnp.exp(scores), 0.0)
    return (expo * (1.0 / jnp.sum(expo, axis=-1, keepdims=True))).astype(jnp.bfloat16)


def forward_kernel(qkv_ref, row_ref, col_ref, qg_ref, kg_ref, out_ref):
    n, _, rows, _ = qkv_ref.shape
    total = n * rows
    q = qkv_ref[:, 0].reshape(total, HEAD_DIM)
    k = qkv_ref[:, 1].reshape(total, HEAD_DIM)
    v = qkv_ref[:, 2].reshape(total, HEAD_DIM)
    qn = (unit_rows(q)[0] * qg_ref[...]).astype(jnp.bfloat16)
    kn = (unit_rows(k)[0] * kg_ref[...]).astype(jnp.bfloat16)
    same = row_ref[...] == col_ref[...]
    probs = probs_of(qn, kn, same)
    out = mm(probs, v, NN).astype(jnp.bfloat16)
    out_ref[...] = out.reshape(n, rows, HEAD_DIM)


def norm_back(unit, inverse, gain, d_norm):
    part = jnp.sum(unit * d_norm, axis=0, keepdims=True)
    d_unit = d_norm * gain
    d_rows = inverse * (d_unit - unit * jnp.mean(unit * d_unit, axis=-1, keepdims=True))
    return d_rows.astype(jnp.bfloat16), part


def backward_kernel(qkv_ref, row_ref, col_ref, qg_ref, kg_ref, *refs):
    d_refs, (grad_ref, qpart_ref, kpart_ref) = refs[:-3], refs[-3:]
    n, _, rows, _ = qkv_ref.shape
    total = n * rows
    q = qkv_ref[:, 0].reshape(total, HEAD_DIM)
    k = qkv_ref[:, 1].reshape(total, HEAD_DIM)
    v = qkv_ref[:, 2].reshape(total, HEAD_DIM)
    q_unit, q_inv = unit_rows(q)
    k_unit, k_inv = unit_rows(k)
    qg, kg = qg_ref[...], kg_ref[...]
    qn = (q_unit * qg).astype(jnp.bfloat16)
    kn = (k_unit * kg).astype(jnp.bfloat16)
    probs = probs_of(qn, kn, row_ref[...] == col_ref[...])
    pieces = []
    for ref in d_refs:
        piece = ref[0].astype(jnp.float32)
        for source in range(1, ref.shape[0]):
            piece = piece + ref[source].astype(jnp.float32)
        pieces.append(piece)
    d_attn = jnp.concatenate(pieces, axis=1).reshape(total, HEAD_DIM).astype(jnp.bfloat16)
    d_probs = mm(d_attn, v, NT)
    probs32 = probs.astype(jnp.float32)
    row_sum = jnp.sum(probs32 * d_probs, axis=-1, keepdims=True)
    d_scores = (probs32 * (d_probs - row_sum) * SCALE).astype(jnp.bfloat16)
    d_value = mm(probs, d_attn, TN).astype(jnp.bfloat16)
    d_query, qpart = norm_back(q_unit, q_inv, qg, mm(d_scores, kn, NN))
    d_key, kpart = norm_back(k_unit, k_inv, kg, mm(d_scores, qn, TN))
    grad_ref[:, 0] = d_query.reshape(n, rows, HEAD_DIM)
    grad_ref[:, 1] = d_key.reshape(n, rows, HEAD_DIM)
    grad_ref[:, 2] = d_value.reshape(n, rows, HEAD_DIM)

    @pl.when(pl.program_id(0) == 0)
    def _():
        qpart_ref[...] = jnp.zeros_like(qpart_ref)
        kpart_ref[...] = jnp.zeros_like(kpart_ref)

    qpart_ref[...] += qpart
    kpart_ref[...] += kpart


def local(
    query_rows, key_rows, value_rows, out_grad, clip_lengths, out_weight, query_gain, key_gain,
    n, groups,
):
    rows, inner = query_rows.shape[1:]
    width = inner // n
    heads = width // HEAD_DIM
    total = n * rows
    columns = out_grad.shape[2] // groups
    piece = rows // CHUNKS

    parts = out_grad[0].reshape(rows, groups, columns).transpose(1, 0, 2)
    parts = lax.all_to_all(parts, "dp", split_axis=0, concat_axis=0, tiled=True)
    qkv = jnp.stack([query_rows[0], key_rows[0], value_rows[0]])
    qkv = qkv.reshape(3, rows, n, width).transpose(2, 0, 1, 3)
    qkv = lax.all_to_all(qkv, "seq", split_axis=0, concat_axis=0, tiled=True)

    seg = segment_ids(clip_lengths[0], total)
    seg_row, seg_col = seg[:, None], seg[None, :]
    qg, kg = query_gain[None], key_gain[None]
    qkv_spec = pl.BlockSpec((n, 3, rows, HEAD_DIM), lambda h: (0, 0, 0, h))
    small = [
        pl.BlockSpec((total, 1), lambda h: (0, 0)),
        pl.BlockSpec((1, total), lambda h: (0, 0)),
        pl.BlockSpec((1, HEAD_DIM), lambda h: (0, 0)),
        pl.BlockSpec((1, HEAD_DIM), lambda h: (0, 0)),
    ]
    params = pltpu.CompilerParams(
        dimension_semantics=("arbitrary",), vmem_limit_bytes=60 * 1024 * 1024
    )
    square = total * total * heads
    attn = pl.pallas_call(
        forward_kernel,
        grid=(heads,),
        in_specs=[qkv_spec] + small,
        out_specs=pl.BlockSpec((n, rows, HEAD_DIM), lambda h: (0, 0, h)),
        out_shape=jax.ShapeDtypeStruct((n, rows, width), jnp.bfloat16),
        compiler_params=params,
        cost_estimate=pl.CostEstimate(
            flops=4 * square * HEAD_DIM, bytes_accessed=8 * total * width, transcendentals=square
        ),
        name="forward",
    )(qkv, seg_row, seg_col, qg, kg)
    attn_all = lax.all_to_all(
        jnp.broadcast_to(attn[None], (groups,) + attn.shape),
        "dp", split_axis=0, concat_axis=0, tiled=True,
    )

    start = lax.axis_index("dp") * columns
    weight = lax.dynamic_slice_in_dim(out_weight, start, columns, 1)
    weight_raw = jnp.zeros((width, columns), jnp.float32)
    d_parts = []
    for j in range(CHUNKS):
        mine = lax.slice_in_dim(parts, j * piece, (j + 1) * piece, axis=1)
        full = lax.all_gather(mine, "seq", axis=1)
        partial = jnp.einsum(
            "gtrc,hc->gtrh", full, weight, preferred_element_type=jnp.float32
        ).astype(jnp.bfloat16)
        d_parts.append(lax.all_to_all(partial, "dp", split_axis=0, concat_axis=0, tiled=True))
        slab = lax.slice_in_dim(attn_all, j * piece, (j + 1) * piece, axis=2)
        weight_raw = weight_raw + jnp.einsum(
            "gtrh,gtrc->hc", slab, full, preferred_element_type=jnp.float32
        )

    d_spec = pl.BlockSpec((groups, n, piece, HEAD_DIM), lambda h: (0, 0, 0, h))
    one = pl.BlockSpec((1, HEAD_DIM), lambda h: (0, 0))
    row = jax.ShapeDtypeStruct((1, HEAD_DIM), jnp.float32)
    grads, qpart, kpart = pl.pallas_call(
        backward_kernel,
        grid=(heads,),
        in_specs=[qkv_spec] + small + [d_spec] * CHUNKS,
        out_specs=(qkv_spec, one, one),
        out_shape=(jax.ShapeDtypeStruct((n, 3, rows, width), jnp.bfloat16), row, row),
        compiler_params=params,
        cost_estimate=pl.CostEstimate(
            flops=12 * square * HEAD_DIM, bytes_accessed=28 * total * width, transcendentals=square
        ),
        name="backward",
    )(qkv, seg_row, seg_col, qg, kg, *d_parts)
    back = lax.all_to_all(grads, "seq", split_axis=0, concat_axis=0, tiled=True)
    query_back, key_back, value_back = (
        back[:, i].transpose(1, 0, 2).reshape(1, rows, inner) for i in range(3)
    )

    packed = jnp.concatenate(
        [qpart[0], kpart[0], jnp.full((HEAD_DIM,), jnp.sum(weight_raw * weight_raw))]
    )
    packed = lax.psum(packed, ("dp", "seq"))
    qgain_raw, kgain_raw = packed[:HEAD_DIM], packed[HEAD_DIM : 2 * HEAD_DIM]
    squares = (
        packed[2 * HEAD_DIM] + jnp.sum(qgain_raw * qgain_raw) + jnp.sum(kgain_raw * kgain_raw)
    )
    grad_norm = jnp.sqrt(squares)
    factor = jnp.minimum(jnp.float32(1.0), MAX_NORM / (grad_norm + EPS))
    return (
        query_back,
        key_back,
        value_back,
        weight_raw * factor,
        qgain_raw * factor,
        kgain_raw * factor,
        grad_norm,
    )


def solution(mesh):
    rows = P("dp", "seq", None)
    return jax.shard_map(
        functools.partial(local, n=mesh.shape["seq"], groups=mesh.shape["dp"]),
        mesh=mesh,
        in_specs=(rows, rows, rows, rows, P("dp", None), P("seq", None), P(), P()),
        out_specs=(rows, rows, rows, P("seq", "dp"), P(), P(), P()),
        check_vma=False,
    )
```

```python
import functools

import jax
import jax.numpy as jnp
from jax import lax
from jax.experimental import pallas as pl
from jax.experimental.pallas import tpu as pltpu
from jax.sharding import PartitionSpec as P

HEAD_DIM = 128
MAX_NORM = 768
EPS = 1e-06
SCALE = HEAD_DIM ** (-0.5)
NT = (((1,), (1,)), ((), ()))
TN = (((0,), (0,)), ((), ()))
NN = (((1,), (0,)), ((), ()))


def mm(a, b, dims):
    return lax.dot_general(a, b, dims, preferred_element_type=jnp.float32)


def segment_ids(lengths, total):
    ends = jnp.cumsum(lengths)
    places = jnp.arange(total, dtype=jnp.int32)
    return jnp.sum((places[:, None] >= ends[None, :]).astype(jnp.int32), axis=1)


def unit_rows(rows):
    wide = rows.astype(jnp.float32)
    inverse = lax.rsqrt(jnp.mean(wide * wide, axis=-1, keepdims=True) + EPS)
    return wide * inverse, inverse


def probs_of(qn, kn, same):
    scores = mm(qn, kn, NT) * SCALE
    expo = jnp.where(same, jnp.exp(scores), 0.0)
    return (expo * (1.0 / jnp.sum(expo, axis=-1, keepdims=True))).astype(jnp.bfloat16)


def forward_kernel(q_ref, k_ref, v_ref, row_ref, col_ref, qg_ref, kg_ref, out_ref):
    qn = (unit_rows(q_ref[...])[0] * qg_ref[...]).astype(jnp.bfloat16)
    kn = (unit_rows(k_ref[...])[0] * kg_ref[...]).astype(jnp.bfloat16)
    probs = probs_of(qn, kn, row_ref[...] == col_ref[...])
    out_ref[...] = mm(probs, v_ref[...], NN).astype(jnp.bfloat16)


def norm_back(unit, inverse, gain, d_norm):
    part = jnp.sum(unit * d_norm, axis=0, keepdims=True)
    d_unit = d_norm * gain
    d_rows = inverse * (d_unit - unit * jnp.mean(unit * d_unit, axis=-1, keepdims=True))
    return d_rows.astype(jnp.bfloat16), part


def backward_kernel(
    q_ref, k_ref, v_ref, row_ref, col_ref, qg_ref, kg_ref, d_ref,
    dq_ref, dk_ref, dv_ref, qpart_ref, kpart_ref,
):
    q_unit, q_inv = unit_rows(q_ref[...])
    k_unit, k_inv = unit_rows(k_ref[...])
    qg, kg = qg_ref[...], kg_ref[...]
    qn = (q_unit * qg).astype(jnp.bfloat16)
    kn = (k_unit * kg).astype(jnp.bfloat16)
    probs = probs_of(qn, kn, row_ref[...] == col_ref[...])
    d_attn = d_ref[...]
    d_probs = mm(d_attn, v_ref[...], NT)
    probs32 = probs.astype(jnp.float32)
    row_sum = jnp.sum(probs32 * d_probs, axis=-1, keepdims=True)
    d_scores = (probs32 * (d_probs - row_sum) * SCALE).astype(jnp.bfloat16)
    dv_ref[...] = mm(probs, d_attn, TN).astype(jnp.bfloat16)
    dq_ref[...], qpart = norm_back(q_unit, q_inv, qg, mm(d_scores, kn, NN))
    dk_ref[...], kpart = norm_back(k_unit, k_inv, kg, mm(d_scores, qn, TN))

    @pl.when(pl.program_id(0) == 0)
    def _():
        qpart_ref[...] = jnp.zeros_like(qpart_ref)
        kpart_ref[...] = jnp.zeros_like(kpart_ref)

    qpart_ref[...] += qpart
    kpart_ref[...] += kpart


def sum_kernel(axis, size, x_ref, out_ref, held, send_sem, recv_sem):
    me = lax.axis_index(axis)
    peers = [lax.rem(me + step, size) for step in range(1, size)]
    barrier = pltpu.get_barrier_semaphore()
    for peer in peers:
        pl.semaphore_signal(
            barrier, inc=1, device_id={axis: peer}, device_id_type=pl.DeviceIdType.MESH
        )
    pl.semaphore_wait(barrier, size - 1)
    copies = [
        pltpu.make_async_remote_copy(
            src_ref=x_ref,
            dst_ref=held.at[me],
            send_sem=send_sem.at[step],
            recv_sem=recv_sem.at[step],
            device_id={axis: peer},
            device_id_type=pl.DeviceIdType.MESH,
        )
        for step, peer in enumerate(peers)
    ]
    for copy in copies:
        copy.start()
    held[me] = x_ref[...]
    for copy in copies:
        copy.wait()
    total = held[0]
    for source in range(1, size):
        total = total + held[source]
    out_ref[...] = total


def sum_over(x, axis, size, collective_id):
    return pl.pallas_call(
        functools.partial(sum_kernel, axis, size),
        in_specs=[pl.BlockSpec(memory_space=pltpu.VMEM)],
        out_specs=pl.BlockSpec(memory_space=pltpu.VMEM),
        out_shape=jax.ShapeDtypeStruct(x.shape, x.dtype),
        scratch_shapes=[
            pltpu.VMEM((size,) + x.shape, x.dtype),
            pltpu.SemaphoreType.DMA((size - 1,)),
            pltpu.SemaphoreType.DMA((size - 1,)),
        ],
        compiler_params=pltpu.CompilerParams(
            collective_id=collective_id, has_side_effects=True
        ),
        name="sum_" + axis,
    )(x)


def local(
    query_rows, key_rows, value_rows, out_grad, clip_lengths, out_weight, query_gain, key_gain,
    n, groups,
):
    rows, inner = query_rows.shape[1:]
    width = inner // n
    heads = width // HEAD_DIM
    total = n * rows

    qkv = [
        lax.all_to_all(x[0], "seq", split_axis=1, concat_axis=0, tiled=True)
        for x in (query_rows, key_rows, value_rows)
    ]
    out_full = lax.all_gather(out_grad[0], "seq", axis=0, tiled=True)
    seg = segment_ids(clip_lengths[0], total)
    shared = [seg[:, None], seg[None, :], query_gain[None], key_gain[None]]
    head = pl.BlockSpec((total, HEAD_DIM), lambda h: (0, h))
    one = pl.BlockSpec((1, HEAD_DIM), lambda h: (0, 0))
    small = [
        pl.BlockSpec((total, 1), lambda h: (0, 0)),
        pl.BlockSpec((1, total), lambda h: (0, 0)),
        one,
        one,
    ]
    params = pltpu.CompilerParams(
        dimension_semantics=("arbitrary",), vmem_limit_bytes=60 * 1024 * 1024
    )
    square = total * total * heads
    flat = jax.ShapeDtypeStruct((total, width), jnp.bfloat16)
    attn = pl.pallas_call(
        forward_kernel,
        grid=(heads,),
        in_specs=[head] * 3 + small,
        out_specs=head,
        out_shape=flat,
        compiler_params=params,
        cost_estimate=pl.CostEstimate(
            flops=4 * square * HEAD_DIM, bytes_accessed=8 * total * width, transcendentals=square
        ),
        name="forward",
    )(*qkv, *shared)
    weight_part = lax.dot_general(attn, out_full, TN, preferred_element_type=jnp.float32)
    weight_shard = lax.psum_scatter(
        weight_part.astype(jnp.bfloat16), "dp", scatter_dimension=1, tiled=True
    ).astype(jnp.float32)
    d_attn = mm(out_full, out_weight, NT).astype(jnp.bfloat16)
    row = jax.ShapeDtypeStruct((1, HEAD_DIM), jnp.float32)
    *grads, qpart, kpart = pl.pallas_call(
        backward_kernel,
        grid=(heads,),
        in_specs=[head] * 3 + small + [head],
        out_specs=(head, head, head, one, one),
        out_shape=(flat, flat, flat, row, row),
        compiler_params=params,
        cost_estimate=pl.CostEstimate(
            flops=12 * square * HEAD_DIM, bytes_accessed=14 * total * width, transcendentals=square
        ),
        name="backward",
    )(*qkv, *shared, d_attn)
    query_back, key_back, value_back = (
        lax.all_to_all(x, "seq", split_axis=0, concat_axis=1, tiled=True)[None] for x in grads
    )

    level = jnp.full((6, HEAD_DIM), jnp.sum(weight_shard * weight_shard))
    packed = jnp.concatenate([qpart, kpart, level])
    packed = sum_over(sum_over(packed, "dp", groups, 0), "seq", n, 1)
    qgain_raw, kgain_raw = packed[0], packed[1]
    squares = packed[2, 0] + jnp.sum(qgain_raw * qgain_raw) + jnp.sum(kgain_raw * kgain_raw)
    grad_norm = jnp.sqrt(squares)
    factor = jnp.minimum(jnp.float32(1.0), MAX_NORM / (grad_norm + EPS))
    return (
        query_back,
        key_back,
        value_back,
        weight_shard * factor,
        qgain_raw * factor,
        kgain_raw * factor,
        grad_norm,
    )


def solution(mesh):
    rows = P("dp", "seq", None)
    return jax.shard_map(
        functools.partial(local, n=mesh.shape["seq"], groups=mesh.shape["dp"]),
        mesh=mesh,
        in_specs=(rows, rows, rows, rows, P("dp", None), P("seq", None), P(), P()),
        out_specs=(rows, rows, rows, P("seq", "dp"), P(), P(), P()),
        check_vma=False,
    )
```
